32 devices in a mesh: fsdp: 4 (over x, core), tm: 8 (over z, y).
Axes of the slice: x: 2, y: 2, z: 4, core: 2. Of those that a mesh axis runs over, the one named last changes fastest.
Arguments:
- tokens: bfloat16 [8, 8, 256, 1024], P('fsdp', 'tm'), may hold values from -6 to 6
- spatial_gain: float32 [1024], replicated, may hold values from 0.25 to 1.75
- spatial_qkv: bfloat16 [1024, 1536], P('fsdp'), may hold values from -16 to 16
- spatial_out: bfloat16 [512, 1024], P('fsdp'), may hold values from -0.25 to 0.25
- temporal_gain: float32 [1024], replicated, may hold values from 0.25 to 1.75
- temporal_qkv: bfloat16 [1024, 1536], P('fsdp'), may hold values from -16 to 16
- temporal_out: bfloat16 [512, 1024], P('fsdp'), may hold values from -0.25 to 0.25
Outputs:
- encoded: bfloat16 [8, 8, 256, 1024], P('fsdp', 'tm')
The draws below stay inside these ranges and needn't reach their ends.
All inputs are finite; a program needn't handle non-finite values.
Results may differ from the reference program's by a relative error of at most 0.0061.
Values may be sent and summed in bfloat16 or wider, within the bound.
A program may use at most 64 MiB of HBM per device.

```python
import jax
import jax.numpy as jnp
from jax import lax

D = 1024
HEAD = 64
HEADS = 8
P_SIZE = 256
INNER = 512
CLIPS = 8
FRAMES = 8


def drawn_weight(key):
    column_count = 3 * INNER
    sample = jax.random.normal(key, (D, column_count), jnp.float32) * D ** (-0.5)
    return jnp.clip(sample, -16.0, 16.0)


def draw_spatial_qkv(key, part):
    return drawn_weight(jax.random.fold_in(key, 11)).astype(jnp.bfloat16)


def draw_temporal_qkv(key, part):
    return drawn_weight(jax.random.fold_in(key, 23)).astype(jnp.bfloat16)


def draw_tokens(key, part):
    sample = jax.random.normal(jax.random.fold_in(key, 5), (CLIPS, FRAMES, P_SIZE, D), jnp.float32)
    return jnp.clip(sample, -6.0, 6.0).astype(jnp.bfloat16)


def shard_levels(rng, dims, shards, least, high):
    level, own = 1.0, jax.random.fold_in(rng, 6)
    for dim, parts in shards:
        heights = jnp.exp(jax.random.uniform(jax.random.fold_in(own, dim), (parts,), jnp.float32, least / len(shards), high / len(shards)))
        level = level * jnp.repeat(heights, dims[dim] // parts).reshape([-1 if axis == dim else 1 for axis in range(len(dims))])
    return level


def bell_draw(key, shape, scale, reach, cuts=(), dtype=jnp.bfloat16):
    level = shard_levels(key, shape, cuts, -0.22, 0.18) if cuts else 1.0
    result = jax.random.normal(key, shape, jnp.float32) * scale * level
    return jnp.minimum(jnp.maximum(result, -reach), reach).astype(dtype)


def setup_inputs(seed: int = 0) -> dict:
    arg_keys = jax.random.split(jax.random.key(seed), 8)
    return {
        "tokens": draw_tokens(jax.random.fold_in(arg_keys[7], 71), 0),
        "spatial_gain": jnp.clip(1.0 + 0.15 * jax.random.normal(arg_keys[1], (D,), jnp.float32), 0.25, 1.75),
        "spatial_qkv": draw_spatial_qkv(jax.random.fold_in(arg_keys[7], 71), 0),
        "spatial_out": bell_draw(arg_keys[3], (INNER, D), INNER ** -0.5, 0.25, ((0, 4),)),
        "temporal_gain": jnp.clip(1.0 + 0.15 * jax.random.normal(arg_keys[4], (D,), jnp.float32), 0.25, 1.75),
        "temporal_qkv": draw_temporal_qkv(jax.random.fold_in(arg_keys[7], 71), 0),
        "temporal_out": bell_draw(arg_keys[6], (INNER, D), INNER ** -0.5, 0.25, ((0, 4),)),
    }


EPSILON = 1e-06

def norm_rows(source, norm_gain):
    values = source.astype(jnp.float32)
    centre = values - lax.optimization_barrier(jnp.mean(values, axis=-1, keepdims=True))
    spread = lax.optimization_barrier(jnp.mean(centre * centre, axis=-1, keepdims=True))
    return (centre * lax.rsqrt(spread + EPSILON) * norm_gain).astype(jnp.bfloat16)

def attention_core(projected):
    inner_width = projected.shape[-1] // 3
    lead_shape = projected.shape[:-1]
    queries = projected[..., :inner_width].reshape(lead_shape + (HEADS, HEAD))
    key_rows = projected[..., inner_width:2 * inner_width].reshape(lead_shape + (HEADS, HEAD))
    value_rows = projected[..., 2 * inner_width:].astype(jnp.bfloat16).reshape(lead_shape + (HEADS, HEAD))
    scores = jnp.einsum('blmhe,bkmhe->bmhlk', queries, key_rows, precision=lax.Precision.HIGHEST) * HEAD ** (-0.5)
    row_max = lax.optimization_barrier(jnp.max(scores, axis=-1, keepdims=True))
    exponent = jnp.exp(scores - row_max)
    weights = (exponent / lax.optimization_barrier(jnp.sum(exponent, axis=-1, keepdims=True))).astype(jnp.bfloat16)
    context = jnp.einsum('bmhlk,bkmhe->blmhe', weights.astype(jnp.float32), value_rows.astype(jnp.float32), precision=lax.Precision.HIGHEST)
    return context.astype(jnp.bfloat16).reshape(lead_shape + (inner_width,))

def reference(tokens, spatial_gain, spatial_qkv, spatial_out, temporal_gain, temporal_qkv, temporal_out):

    def encode_clip(clip_tokens):
        frame_count, place_count, feature_width = clip_tokens.shape
        normed = norm_rows(clip_tokens, spatial_gain).reshape(-1, feature_width)
        projected = jnp.dot(normed, spatial_qkv, preferred_element_type=jnp.float32)
        context = attention_core(projected.reshape(frame_count, place_count, 1, 3 * INNER)).reshape(-1, INNER)
        middle = (clip_tokens.astype(jnp.float32).reshape(-1, feature_width) + jnp.dot(context, spatial_out, preferred_element_type=jnp.float32)).astype(jnp.bfloat16)
        normed_t = norm_rows(middle, temporal_gain)
        projected_t = jnp.dot(normed_t, temporal_qkv, preferred_element_type=jnp.float32)
        context_t = attention_core(projected_t.reshape(1, frame_count, place_count, 3 * INNER)).reshape(-1, INNER)
        encoded = middle.astype(jnp.float32) + jnp.dot(context_t, temporal_out, preferred_element_type=jnp.float32)
        return encoded.astype(jnp.bfloat16).reshape(frame_count, place_count, feature_width)
    return lax.map(encode_clip, tokens)
```

```python
import functools

import jax
import jax.numpy as jnp
from jax import lax
from jax.experimental import pallas as pl
from jax.experimental.pallas import tpu as pltpu
from jax.sharding import PartitionSpec as P

HEAD = 64
LANES = 128
EPSILON = 1e-06
MESH = pl.DeviceIdType.MESH
BF16 = jnp.bfloat16
F32 = jnp.float32


def pieces_of(depth):
    return max(1, depth // 64)


def kernel(
    n_f, n_t, tok, sg, sqkv, sout, tg, tqkv, tout, out,
    xv, normed, proj, ctx, mid, arrived, ctx_t, ctx_back, wsq, wso, wtq, wto, outv,
    local_sem, w_local, w_send, w_recv, m_send, m_recv, o_send, o_recv,
    a_send, a_recv, c_send, c_recv, own_sem, out_sem,
):
    f = lax.axis_index("fsdp")
    t = lax.axis_index("tm")
    mate = f + 1 - 2 * (f % 2)
    peers = n_f // 2 - 1
    clips = xv.shape[0]
    rows, width = xv.shape[1:]
    places = rows // n_t
    inner = wso.shape[0]

    barrier = pltpu.get_barrier_semaphore()
    pl.semaphore_signal(barrier, inc=1, device_id={"fsdp": mate}, device_id_type=MESH)
    for k in range(1, peers + 1):
        pl.semaphore_signal(
            barrier, inc=1, device_id={"fsdp": (f + 2 * k) % n_f}, device_id_type=MESH
        )
    for j in range(1, n_t):
        pl.semaphore_signal(
            barrier, inc=1, device_id={"tm": (t + j) % n_t}, device_id_type=MESH
        )

    token_copy = pltpu.make_async_copy(tok, xv, local_sem)
    token_copy.start()
    weights = ((sqkv, wsq), (sout, wso), (tqkv, wtq), (tout, wto))
    own_weights = []
    for w, (src, dst) in enumerate(weights):
        depth = src.shape[0]
        cp = pltpu.make_async_copy(src, dst.at[pl.ds(f * depth, depth)], w_local.at[w])
        cp.start()
        own_weights.append(cp)

    pl.semaphore_wait(barrier, 1 + peers + n_t - 1)

    sends = []

    def peer_copy(w, k, p, source):
        src, dst = weights[w]
        depth = src.shape[0]
        size = depth // pieces_of(depth)
        return pltpu.make_async_remote_copy(
            src_ref=src.at[pl.ds(p * size, size)],
            dst_ref=dst.at[pl.ds(pl.multiple_of(source * depth + p * size, size), size)],
            send_sem=w_send.at[w, k, p],
            recv_sem=w_recv.at[w, k, p],
            device_id={"fsdp": (f + 2 * (k + 1)) % n_f},
            device_id_type=MESH,
        )

    def mate_own(w, source):
        src, dst = weights[w]
        depth = src.shape[0]
        return pltpu.make_async_remote_copy(
            src_ref=src,
            dst_ref=dst.at[pl.ds(pl.multiple_of(source * depth, depth), depth)],
            send_sem=o_send.at[w],
            recv_sem=o_recv.at[w],
            device_id={"fsdp": mate},
            device_id_type=MESH,
        )

    def mate_forward(w, k, p, source):
        src, dst = weights[w]
        depth = src.shape[0]
        size = depth // pieces_of(depth)
        where = pl.ds(pl.multiple_of(source * depth + p * size, size), size)
        return pltpu.make_async_remote_copy(
            src_ref=dst.at[where],
            dst_ref=dst.at[where],
            send_sem=m_send.at[w, k, p],
            recv_sem=m_recv.at[w, k, p],
            device_id={"fsdp": mate},
            device_id_type=MESH,
        )

    for w, (src, dst) in enumerate(weights):
        for p in range(pieces_of(src.shape[0])):
            for k in range(peers):
                cp = peer_copy(w, k, p, f)
                cp.start()
                sends.append(cp)
        cp = mate_own(w, f)
        cp.start()
        sends.append(cp)

    def relay(w):
        for p in range(pieces_of(weights[w][0].shape[0])):
            for k in range(peers):
                source = (f + n_f - 2 * (k + 1)) % n_f
                peer_copy(w, k, p, source).wait_recv()
                cp = mate_forward(w, k, p, source)
                cp.start()
                sends.append(cp)

    def gathered(w):
        own_weights[w].wait()
        mate_own(w, mate).wait_recv()
        for p in range(pieces_of(weights[w][0].shape[0])):
            for k in range(peers):
                mate_forward(w, k, p, (mate + n_f - 2 * (k + 1)) % n_f).wait_recv()

    def norm(values, gain):
        centre = values - jnp.mean(values, axis=-1, keepdims=True)
        spread = jnp.mean(centre * centre, axis=-1, keepdims=True)
        return (centre * lax.rsqrt(spread + EPSILON) * gain).astype(BF16)

    def project(c, weight):
        tile = inner

        @pl.loop(0, weight.shape[1] // tile)
        def _(i):
            cols = pl.ds(pl.multiple_of(i * tile, LANES), tile)
            part = jnp.dot(normed[c], weight[:, cols], preferred_element_type=F32)
            proj[c, :, :, cols] = part.reshape(n_t, places, tile)

    def attend(c, lo, group, count, masked, store):
        size = n_t * group
        lane = lax.broadcasted_iota(jnp.int32, (1, LANES), 1)
        first = lane < HEAD

        @pl.loop(0, inner // LANES)
        def _(i):
            def read(offset):
                cols = pl.ds(pl.multiple_of(offset + i * LANES, LANES), LANES)
                return proj[c, :, lo : lo + group, cols].reshape(size, LANES)

            q = read(0) * HEAD ** (-0.5)
            k = read(inner)
            v = read(2 * inner).astype(BF16)
            kh = k.astype(BF16)
            kl = (k - kh.astype(F32)).astype(BF16)
            kk = jnp.concatenate([kh, kh], axis=1)
            parts = []
            for h in range(LANES // HEAD):
                qm = jnp.where(first == (h == 0), q, 0.0)
                qh = qm.astype(BF16)
                ql = (qm - qh.astype(F32)).astype(BF16)
                qq = jnp.concatenate([qh, ql], axis=1)
                dims = (((1,), (1,)), ((), ()))
                s = lax.dot_general(qq, kk, dims, preferred_element_type=F32)
                s = s + lax.dot_general(qh, kl, dims, preferred_element_type=F32)
                if masked:
                    r = lax.broadcasted_iota(jnp.int32, (size, size), 0)
                    l = lax.broadcasted_iota(jnp.int32, (size, size), 1)
                    s = jnp.where(lax.rem(r, group) == lax.rem(l, group), s, -1e30)
                e = jnp.exp(s - jnp.max(s, axis=-1, keepdims=True))
                total = jnp.sum(e, axis=-1, keepdims=True)
                pv = jnp.dot(e.astype(BF16), v, preferred_element_type=F32)
                parts.append(pv / total)
            result = jnp.where(first, parts[0], parts[1])
            store(pl.ds(pl.multiple_of(i * LANES, LANES), LANES), result)

    def a2a(c, j, slot_from, send):
        to = (t + j) % n_t
        return pltpu.make_async_remote_copy(
            src_ref=mid.at[c, to],
            dst_ref=arrived.at[c, slot_from],
            send_sem=a_send.at[c, j],
            recv_sem=a_recv.at[c, j],
            device_id={"tm": to},
            device_id_type=MESH,
        )

    def back(c, j, slot_from):
        to = (t + j) % n_t
        return pltpu.make_async_remote_copy(
            src_ref=ctx_t.at[c, to],
            dst_ref=ctx_back.at[c, slot_from],
            send_sem=c_send.at[c, j],
            recv_sem=c_recv.at[c, j],
            device_id={"tm": to},
            device_id_type=MESH,
        )

    token_copy.wait()
    block = min(rows, 64)
    for c in range(clips):

        @pl.loop(0, rows // block)
        def _(i):
            where = pl.ds(pl.multiple_of(i * block, block), block)
            normed[c, where] = norm(xv[c, where].astype(F32), sg[...])

    relay(0)
    gathered(0)
    for c in range(clips):
        project(c, wsq)
    own_copies = []
    for c in range(clips):

        def store_spatial(cols, result):
            ctx[:, cols] = result.astype(BF16)

        attend(c, 0, places, 1, False, store_spatial)
        if c == 0:
            relay(1)
            gathered(1)

        @pl.loop(0, width // inner)
        def _(i):
            cols = pl.ds(pl.multiple_of(i * inner, LANES), inner)
            part = xv[c, :, cols].astype(F32) + jnp.dot(
                ctx[...], wso[:, cols], preferred_element_type=F32
            )
            mid[c, :, :, cols] = part.reshape(n_t, places, inner).astype(BF16)

        for j in range(1, n_t):
            cp = a2a(c, j, t, True)
            cp.start()
            sends.append(cp)
        cp = pltpu.make_async_copy(mid.at[c, t], arrived.at[c, t], own_sem.at[0, c])
        cp.start()
        own_copies.append(cp)

    relay(2)
    own_back = []
    group = min(places, 16)
    for c in range(clips):
        own_copies[c].wait()
        for j in range(1, n_t):
            a2a(c, j, (t + n_t - j) % n_t, False).wait_recv()
        step = max(1, block // places)

        @pl.loop(0, n_t // step)
        def _(i):
            values = arrived[c, pl.ds(i * step, step)].astype(F32).reshape(step * places, width)
            where = pl.ds(pl.multiple_of(i * step * places, step * places), step * places)
            normed[c, where] = norm(values, tg[...])

        if c == 0:
            gathered(2)
        project(c, wtq)
        for g in range(places // group):

            def store_temporal(cols, result):
                ctx_t[c, :, g * group : (g + 1) * group, cols] = result.reshape(
                    n_t, group, LANES
                ).astype(BF16)

            attend(c, g * group, group, n_t, True, store_temporal)
        for j in range(1, n_t):
            cp = back(c, j, t)
            cp.start()
            sends.append(cp)
        cp = pltpu.make_async_copy(ctx_t.at[c, t], ctx_back.at[c, t], own_sem.at[1, c])
        cp.start()
        own_back.append(cp)
        if c == 0:
            relay(3)
    gathered(3)
    finals = []
    for c in range(clips):
        own_back[c].wait()
        for j in range(1, n_t):
            back(c, j, (t + n_t - j) % n_t).wait_recv()
        ctx[...] = ctx_back[c].astype(F32).reshape(rows, inner).astype(BF16)

        @pl.loop(0, width // inner)
        def _(i):
            cols = pl.ds(pl.multiple_of(i * inner, LANES), inner)
            part = mid[c, :, :, cols].astype(F32).reshape(rows, inner) + jnp.dot(
                ctx[...], wto[:, cols], preferred_element_type=F32
            )
            outv[c, :, cols] = part.astype(BF16)

        cp = pltpu.make_async_copy(outv.at[c], out.at[c], out_sem.at[c])
        cp.start()
        finals.append(cp)
    for cp in sends:
        cp.wait_send()
    for cp in finals:
        cp.wait()


def shards(
    n_f, n_t, tokens, spatial_gain, spatial_qkv, spatial_out, temporal_gain, temporal_qkv,
    temporal_out,
):
    clip_count, frames, rows, width = tokens.shape
    assert frames == 1
    inner = spatial_out.shape[0] * n_f
    columns = spatial_qkv.shape[1]
    places = rows // n_t
    peers = max(1, n_f // 2 - 1)
    most = pieces_of(max(spatial_qkv.shape[0], spatial_out.shape[0]))
    anywhere = pl.BlockSpec(memory_space=pl.ANY)
    vmem = pl.BlockSpec(memory_space=pltpu.VMEM)
    dma = pltpu.SemaphoreType.DMA
    result = pl.pallas_call(
        functools.partial(kernel, n_f, n_t),
        out_shape=jax.ShapeDtypeStruct((clip_count, rows, width), BF16),
        in_specs=[anywhere, vmem, anywhere, anywhere, vmem, anywhere, anywhere],
        out_specs=anywhere,
        scratch_shapes=[
            pltpu.VMEM((clip_count, rows, width), BF16),
            pltpu.VMEM((clip_count, rows, width), BF16),
            pltpu.VMEM((clip_count, n_t, places, columns), F32),
            pltpu.VMEM((rows, inner), BF16),
            pltpu.VMEM((clip_count, n_t, places, width), BF16),
            pltpu.VMEM((clip_count, n_t, places, width), BF16),
            pltpu.VMEM((clip_count, n_t, places, inner), BF16),
            pltpu.VMEM((clip_count, n_t, places, inner), BF16),
            pltpu.VMEM((width, columns), BF16),
            pltpu.VMEM((inner, width), BF16),
            pltpu.VMEM((width, columns), BF16),
            pltpu.VMEM((inner, width), BF16),
            pltpu.VMEM((clip_count, rows, width), BF16),
            dma,
            dma((4,)),
            dma((4, peers, most)),
            dma((4, peers, most)),
            dma((4, peers, most)),
            dma((4, peers, most)),
            dma((4,)),
            dma((4,)),
            dma((clip_count, n_t)),
            dma((clip_count, n_t)),
            dma((clip_count, n_t)),
            dma((clip_count, n_t)),
            dma((2, clip_count)),
            dma((clip_count,)),
        ],
        compiler_params=pltpu.CompilerParams(
            collective_id=0, has_side_effects=True, vmem_limit_bytes=50 * 1024 * 1024
        ),
    )(
        tokens.reshape(clip_count, rows, width),
        spatial_gain.reshape(1, width),
        spatial_qkv,
        spatial_out,
        temporal_gain.reshape(1, width),
        temporal_qkv,
        temporal_out,
    )
    return result.reshape(clip_count, frames, rows, width)


def solution(mesh):
    placed = (
        P("fsdp", "tm", None, None),
        P(),
        P("fsdp", None),
        P("fsdp", None),
        P(),
        P("fsdp", None),
        P("fsdp", None),
    )
    body = functools.partial(shards, mesh.shape["fsdp"], mesh.shape["tm"])
    return jax.shard_map(
        body, mesh=mesh, in_specs=placed, out_specs=P("fsdp", "tm", None, None), check_vma=False
    )
```

```python
import functools

import jax
import jax.numpy as jnp
from jax import lax
from jax.experimental import pallas as pl
from jax.experimental.pallas import tpu as pltpu
from jax.sharding import PartitionSpec as P

HEAD = 64
LANES = 128
EPSILON = 1e-06
MESH = pl.DeviceIdType.MESH
BF16 = jnp.bfloat16
F32 = jnp.float32


def pieces_of(depth):
    return max(2, depth // 32)


def kernel(
    n_f, n_t, tok, sg, sqkv, sout, tg, tqkv, tout, out,
    xv, normed, proj, ctx, mid, arrived, ctx_t, ctx_back, wsq, wso, wtq, wto, outv,
    local_sem, w_local, w_send, w_recv, m_send, m_recv, o_send, o_recv,
    a_send, a_recv, c_send, c_recv, own_sem, out_sem,
):
    f = lax.axis_index("fsdp")
    t = lax.axis_index("tm")
    mate = f + 1 - 2 * (f % 2)
    peers = n_f // 2 - 1
    clips = xv.shape[0]
    rows, width = xv.shape[1:]
    places = rows // n_t
    inner = wso.shape[0]

    barrier = pltpu.get_barrier_semaphore()
    pl.semaphore_signal(barrier, inc=1, device_id={"fsdp": mate}, device_id_type=MESH)
    for k in range(1, peers + 1):
        pl.semaphore_signal(
            barrier, inc=1, device_id={"fsdp": (f + 2 * k) % n_f}, device_id_type=MESH
        )
    for j in range(1, n_t):
        pl.semaphore_signal(
            barrier, inc=1, device_id={"tm": (t + j) % n_t}, device_id_type=MESH
        )

    token_copy = pltpu.make_async_copy(tok, xv, local_sem)
    token_copy.start()
    weights = ((sqkv, wsq), (sout, wso), (tqkv, wtq), (tout, wto))
    own_weights = []
    for w, (src, dst) in enumerate(weights):
        depth = src.shape[0]
        cp = pltpu.make_async_copy(src, dst.at[pl.ds(f * depth, depth)], w_local.at[w])
        cp.start()
        own_weights.append(cp)

    pl.semaphore_wait(barrier, 1 + peers + n_t - 1)

    sends = []

    def peer_copy(w, k, p, source):
        src, dst = weights[w]
        depth = src.shape[0]
        size = depth // pieces_of(depth)
        return pltpu.make_async_remote_copy(
            src_ref=src.at[pl.ds(p * size, size)],
            dst_ref=dst.at[pl.ds(pl.multiple_of(source * depth + p * size, size), size)],
            send_sem=w_send.at[w, k, p],
            recv_sem=w_recv.at[w, k, p],
            device_id={"fsdp": (f + 2 * (k + 1)) % n_f},
            device_id_type=MESH,
        )

    def mate_own(w, source):
        src, dst = weights[w]
        depth = src.shape[0]
        return pltpu.make_async_remote_copy(
            src_ref=src,
            dst_ref=dst.at[pl.ds(pl.multiple_of(source * depth, depth), depth)],
            send_sem=o_send.at[w],
            recv_sem=o_recv.at[w],
            device_id={"fsdp": mate},
            device_id_type=MESH,
        )

    def mate_forward(w, k, p, source):
        src, dst = weights[w]
        depth = src.shape[0]
        size = depth // pieces_of(depth)
        where = pl.ds(pl.multiple_of(source * depth + p * size, size), size)
        return pltpu.make_async_remote_copy(
            src_ref=dst.at[where],
            dst_ref=dst.at[where],
            send_sem=m_send.at[w, k, p],
            recv_sem=m_recv.at[w, k, p],
            device_id={"fsdp": mate},
            device_id_type=MESH,
        )

    parity = t % 2
    partner = t + 1 - 2 * parity
    half = pieces_of(sqkv.shape[0]) // 2
    small = sqkv.shape[0] // pieces_of(sqkv.shape[0])

    def half_rows(source, part, i):
        start = source * sqkv.shape[0] + (part * half + i) * small
        return pl.ds(pl.multiple_of(start, small), small)

    def direct(k, i, source):
        return pltpu.make_async_remote_copy(
            src_ref=sqkv.at[pl.ds(pl.multiple_of((parity * half + i) * small, small), small)],
            dst_ref=wsq.at[half_rows(source, parity, i)],
            send_sem=w_send.at[0, k, i],
            recv_sem=w_recv.at[0, k, i],
            device_id={"fsdp": (f + 2 * (k + 1)) % n_f},
            device_id_type=MESH,
        )

    def cross(k, i, source, part):
        return pltpu.make_async_remote_copy(
            src_ref=wsq.at[half_rows(source, part, i)],
            dst_ref=wsq.at[half_rows(source, part, i)],
            send_sem=w_send.at[0, k, half + i],
            recv_sem=w_recv.at[0, k, half + i],
            device_id={"tm": partner},
            device_id_type=MESH,
        )

    def half_forward(k, i, source, part, slot):
        return pltpu.make_async_remote_copy(
            src_ref=wsq.at[half_rows(source, part, i)],
            dst_ref=wsq.at[half_rows(source, part, i)],
            send_sem=m_send.at[0, k, slot],
            recv_sem=m_recv.at[0, k, slot],
            device_id={"fsdp": mate},
            device_id_type=MESH,
        )

    def source_of(who, k):
        return (who + n_f - 2 * (k + 1)) % n_f

    def relay_first():
        for i in range(half + 1):
            for k in range(peers):
                source = source_of(f, k)
                if i < half:
                    direct(k, i, source).wait_recv()
                    for cp in (
                        cross(k, i, source, parity),
                        half_forward(k, i, source, parity, i),
                    ):
                        cp.start()
                        sends.append(cp)
                if i > 0:
                    cross(k, i - 1, source, 1 - parity).wait_recv()
                    cp = half_forward(k, i - 1, source, 1 - parity, half + i - 1)
                    cp.start()
                    sends.append(cp)

    def gathered_first():
        own_weights[0].wait()
        mate_own(0, mate).wait_recv()
        for i in range(half):
            for k in range(peers):
                source = source_of(mate, k)
                half_forward(k, i, source, parity, i).wait_recv()
                half_forward(k, i, source, 1 - parity, half + i).wait_recv()

    for w, (src, dst) in enumerate(weights):
        for p in range(half if w == 0 else pieces_of(src.shape[0])):
            for k in range(peers):
                cp = direct(k, p, f) if w == 0 else peer_copy(w, k, p, f)
                cp.start()
                sends.append(cp)
        cp = mate_own(w, f)
        cp.start()
        sends.append(cp)

    def relay(w):
        for p in range(pieces_of(weights[w][0].shape[0])):
            for k in range(peers):
                source = (f + n_f - 2 * (k + 1)) % n_f
                peer_copy(w, k, p, source).wait_recv()
                cp = mate_forward(w, k, p, source)
                cp.start()
                sends.append(cp)

    def gathered(w):
        own_weights[w].wait()
        mate_own(w, mate).wait_recv()
        for p in range(pieces_of(weights[w][0].shape[0])):
            for k in range(peers):
                mate_forward(w, k, p, (mate + n_f - 2 * (k + 1)) % n_f).wait_recv()

    def norm(values, gain):
        centre = values - jnp.mean(values, axis=-1, keepdims=True)
        spread = jnp.mean(centre * centre, axis=-1, keepdims=True)
        return (centre * lax.rsqrt(spread + EPSILON) * gain).astype(BF16)

    def project(c, weight):
        tile = inner

        @pl.loop(0, weight.shape[1] // tile)
        def _(i):
            cols = pl.ds(pl.multiple_of(i * tile, LANES), tile)
            part = jnp.dot(normed[c], weight[:, cols], preferred_element_type=F32)
            proj[c, :, :, cols] = part.reshape(n_t, places, tile)

    def attend(c, lo, group, count, masked, store):
        size = n_t * group
        lane = lax.broadcasted_iota(jnp.int32, (1, LANES), 1)
        first = lane < HEAD

        @pl.loop(0, inner // LANES)
        def _(i):
            def read(offset):
                cols = pl.ds(pl.multiple_of(offset + i * LANES, LANES), LANES)
                return proj[c, :, lo : lo + group, cols].reshape(size, LANES)

            q = read(0) * HEAD ** (-0.5)
            k = read(inner)
            v = read(2 * inner).astype(BF16)
            kh = k.astype(BF16)
            kl = (k - kh.astype(F32)).astype(BF16)
            kk = jnp.concatenate([kh, kh], axis=1)
            parts = []
            for h in range(LANES // HEAD):
                qm = jnp.where(first == (h == 0), q, 0.0)
                qh = qm.astype(BF16)
                ql = (qm - qh.astype(F32)).astype(BF16)
                qq = jnp.concatenate([qh, ql], axis=1)
                dims = (((1,), (1,)), ((), ()))
                s = lax.dot_general(qq, kk, dims, preferred_element_type=F32)
                s = s + lax.dot_general(qh, kl, dims, preferred_element_type=F32)
                if masked:
                    r = lax.broadcasted_iota(jnp.int32, (size, size), 0)
                    l = lax.broadcasted_iota(jnp.int32, (size, size), 1)
                    s = jnp.where(lax.rem(r, group) == lax.rem(l, group), s, -1e30)
                e = jnp.exp(s - jnp.max(s, axis=-1, keepdims=True))
                total = jnp.sum(e, axis=-1, keepdims=True)
                pv = jnp.dot(e.astype(BF16), v, preferred_element_type=F32)
                parts.append(pv / total)
            result = jnp.where(first, parts[0], parts[1])
            store(pl.ds(pl.multiple_of(i * LANES, LANES), LANES), result)

    def a2a(c, j, slot_from, send):
        to = (t + j) % n_t
        return pltpu.make_async_remote_copy(
            src_ref=mid.at[c, to],
            dst_ref=arrived.at[c, slot_from],
            send_sem=a_send.at[c, j],
            recv_sem=a_recv.at[c, j],
            device_id={"tm": to},
            device_id_type=MESH,
        )

    def back(c, j, slot_from):
        to = (t + j) % n_t
        return pltpu.make_async_remote_copy(
            src_ref=ctx_t.at[c, to],
            dst_ref=ctx_back.at[c, slot_from],
            send_sem=c_send.at[c, j],
            recv_sem=c_recv.at[c, j],
            device_id={"tm": to},
            device_id_type=MESH,
        )

    token_copy.wait()
    block = min(rows, 64)
    for c in range(clips):

        @pl.loop(0, rows // block)
        def _(i):
            where = pl.ds(pl.multiple_of(i * block, block), block)
            normed[c, where] = norm(xv[c, where].astype(F32), sg[...])

    relay_first()
    gathered_first()
    for c in range(clips):
        project(c, wsq)
    own_copies = []
    for c in range(clips):

        def store_spatial(cols, result):
            ctx[:, cols] = result.astype(BF16)

        attend(c, 0, places, 1, False, store_spatial)
        if c == 0:
            relay(1)
            gathered(1)

        @pl.loop(0, width // inner)
        def _(i):
            cols = pl.ds(pl.multiple_of(i * inner, LANES), inner)
            part = xv[c, :, cols].astype(F32) + jnp.dot(
                ctx[...], wso[:, cols], preferred_element_type=F32
            )
            mid[c, :, :, cols] = part.reshape(n_t, places, inner).astype(BF16)

        for j in range(1, n_t):
            cp = a2a(c, j, t, True)
            cp.start()
            sends.append(cp)
        cp = pltpu.make_async_copy(mid.at[c, t], arrived.at[c, t], own_sem.at[0, c])
        cp.start()
        own_copies.append(cp)

    relay(2)
    own_back = []
    group = min(places, 16)
    for c in range(clips):
        own_copies[c].wait()
        for j in range(1, n_t):
            a2a(c, j, (t + n_t - j) % n_t, False).wait_recv()
        step = max(1, block // places)

        @pl.loop(0, n_t // step)
        def _(i):
            values = arrived[c, pl.ds(i * step, step)].astype(F32).reshape(step * places, width)
            where = pl.ds(pl.multiple_of(i * step * places, step * places), step * places)
            normed[c, where] = norm(values, tg[...])

        if c == 0:
            gathered(2)
        project(c, wtq)
        for g in range(places // group):

            def store_temporal(cols, result):
                ctx_t[c, :, g * group : (g + 1) * group, cols] = result.reshape(
                    n_t, group, LANES
                ).astype(BF16)

            attend(c, g * group, group, n_t, True, store_temporal)
        for j in range(1, n_t):
            cp = back(c, j, t)
            cp.start()
            sends.append(cp)
        cp = pltpu.make_async_copy(ctx_t.at[c, t], ctx_back.at[c, t], own_sem.at[1, c])
        cp.start()
        own_back.append(cp)
        if c == 0:
            relay(3)
    gathered(3)
    finals = []
    for c in range(clips):
        own_back[c].wait()
        for j in range(1, n_t):
            back(c, j, (t + n_t - j) % n_t).wait_recv()
        ctx[...] = ctx_back[c].astype(F32).reshape(rows, inner).astype(BF16)

        @pl.loop(0, width // inner)
        def _(i):
            cols = pl.ds(pl.multiple_of(i * inner, LANES), inner)
            part = mid[c, :, :, cols].astype(F32).reshape(rows, inner) + jnp.dot(
                ctx[...], wto[:, cols], preferred_element_type=F32
            )
            outv[c, :, cols] = part.astype(BF16)

        cp = pltpu.make_async_copy(outv.at[c], out.at[c], out_sem.at[c])
        cp.start()
        finals.append(cp)
    for cp in sends:
        cp.wait_send()
    for cp in finals:
        cp.wait()


def shards(
    n_f, n_t, tokens, spatial_gain, spatial_qkv, spatial_out, temporal_gain, temporal_qkv,
    temporal_out,
):
    clip_count, frames, rows, width = tokens.shape
    assert frames == 1
    inner = spatial_out.shape[0] * n_f
    columns = spatial_qkv.shape[1]
    places = rows // n_t
    peers = max(1, n_f // 2 - 1)
    most = pieces_of(max(spatial_qkv.shape[0], spatial_out.shape[0]))
    anywhere = pl.BlockSpec(memory_space=pl.ANY)
    vmem = pl.BlockSpec(memory_space=pltpu.VMEM)
    dma = pltpu.SemaphoreType.DMA
    result = pl.pallas_call(
        functools.partial(kernel, n_f, n_t),
        out_shape=jax.ShapeDtypeStruct((clip_count, rows, width), BF16),
        in_specs=[anywhere, vmem, anywhere, anywhere, vmem, anywhere, anywhere],
        out_specs=anywhere,
        scratch_shapes=[
            pltpu.VMEM((clip_count, rows, width), BF16),
            pltpu.VMEM((clip_count, rows, width), BF16),
            pltpu.VMEM((clip_count, n_t, places, columns), F32),
            pltpu.VMEM((rows, inner), BF16),
            pltpu.VMEM((clip_count, n_t, places, width), BF16),
            pltpu.VMEM((clip_count, n_t, places, width), BF16),
            pltpu.VMEM((clip_count, n_t, places, inner), BF16),
            pltpu.VMEM((clip_count, n_t, places, inner), BF16),
            pltpu.VMEM((width, columns), BF16),
            pltpu.VMEM((inner, width), BF16),
            pltpu.VMEM((width, columns), BF16),
            pltpu.VMEM((inner, width), BF16),
            pltpu.VMEM((clip_count, rows, width), BF16),
            dma,
            dma((4,)),
            dma((4, peers, most)),
            dma((4, peers, most)),
            dma((4, peers, most)),
            dma((4, peers, most)),
            dma((4,)),
            dma((4,)),
            dma((clip_count, n_t)),
            dma((clip_count, n_t)),
            dma((clip_count, n_t)),
            dma((clip_count, n_t)),
            dma((2, clip_count)),
            dma((clip_count,)),
        ],
        compiler_params=pltpu.CompilerParams(
            collective_id=0, has_side_effects=True, vmem_limit_bytes=67000000
        ),
    )(
        tokens.reshape(clip_count, rows, width),
        spatial_gain.reshape(1, width),
        spatial_qkv,
        spatial_out,
        temporal_gain.reshape(1, width),
        temporal_qkv,
        temporal_out,
    )
    return result.reshape(clip_count, frames, rows, width)


def solution(mesh):
    placed = (
        P("fsdp", "tm", None, None),
        P(),
        P("fsdp", None),
        P("fsdp", None),
        P(),
        P("fsdp", None),
        P("fsdp", None),
    )
    body = functools.partial(shards, mesh.shape["fsdp"], mesh.shape["tm"])
    return jax.shard_map(
        body, mesh=mesh, in_specs=placed, out_specs=P("fsdp", "tm", None, None), check_vma=False
    )
```

```python
import functools

import jax
import jax.numpy as jnp
from jax import lax
from jax.experimental import pallas as pl
from jax.experimental.pallas import tpu as pltpu
from jax.sharding import PartitionSpec as P

HEAD = 64
LANES = 128
EPSILON = 1e-06
MESH = pl.DeviceIdType.MESH
BF16 = jnp.bfloat16
F32 = jnp.float32


def pieces_of(depth):
    return max(2, depth // 32)


def kernel(
    n_f, n_t, tok, sg, sqkv, sout, tg, tqkv, tout, out,
    xv, normed, proj, ctx, mid, arrived, ctx_t, ctx_back, wsq, wso, wtq, wto, outv,
    local_sem, w_local, w_send, w_recv, m_send, m_recv, o_send, o_recv,
    a_send, a_recv, c_send, c_recv, own_sem, out_sem,
):
    f = lax.axis_index("fsdp")
    t = lax.axis_index("tm")
    mate = f + 1 - 2 * (f % 2)
    peers = n_f // 2 - 1
    clips = xv.shape[0]
    rows, width = xv.shape[1:]
    places = rows // n_t
    inner = wso.shape[0]

    barrier = pltpu.get_barrier_semaphore()
    pl.semaphore_signal(barrier, inc=1, device_id={"fsdp": mate}, device_id_type=MESH)
    for k in range(1, peers + 1):
        pl.semaphore_signal(
            barrier, inc=1, device_id={"fsdp": (f + 2 * k) % n_f}, device_id_type=MESH
        )
    for j in range(1, n_t):
        pl.semaphore_signal(
            barrier, inc=1, device_id={"tm": (t + j) % n_t}, device_id_type=MESH
        )

    token_copy = pltpu.make_async_copy(tok, xv, local_sem)
    token_copy.start()
    weights = ((sqkv, wsq), (sout, wso), (tqkv, wtq), (tout, wto))
    own_weights = []
    for w, (src, dst) in enumerate(weights):
        depth = src.shape[0]
        cp = pltpu.make_async_copy(src, dst.at[pl.ds(f * depth, depth)], w_local.at[w])
        cp.start()
        own_weights.append(cp)

    pl.semaphore_wait(barrier, 1 + peers + n_t - 1)

    sends = []

    def peer_copy(w, k, p, source):
        src, dst = weights[w]
        depth = src.shape[0]
        size = depth // pieces_of(depth)
        return pltpu.make_async_remote_copy(
            src_ref=src.at[pl.ds(p * size, size)],
            dst_ref=dst.at[pl.ds(pl.multiple_of(source * depth + p * size, size), size)],
            send_sem=w_send.at[w, k, p],
            recv_sem=w_recv.at[w, k, p],
            device_id={"fsdp": (f + 2 * (k + 1)) % n_f},
            device_id_type=MESH,
        )

    def mate_own(w, source):
        src, dst = weights[w]
        depth = src.shape[0]
        return pltpu.make_async_remote_copy(
            src_ref=src,
            dst_ref=dst.at[pl.ds(pl.multiple_of(source * depth, depth), depth)],
            send_sem=o_send.at[w],
            recv_sem=o_recv.at[w],
            device_id={"fsdp": mate},
            device_id_type=MESH,
        )

    def mate_forward(w, k, p, source):
        src, dst = weights[w]
        depth = src.shape[0]
        size = depth // pieces_of(depth)
        where = pl.ds(pl.multiple_of(source * depth + p * size, size), size)
        return pltpu.make_async_remote_copy(
            src_ref=dst.at[where],
            dst_ref=dst.at[where],
            send_sem=m_send.at[w, k, p],
            recv_sem=m_recv.at[w, k, p],
            device_id={"fsdp": mate},
            device_id_type=MESH,
        )

    parity = t % 2
    partner = t + 1 - 2 * parity
    half = pieces_of(sqkv.shape[0]) // 2
    small = sqkv.shape[0] // pieces_of(sqkv.shape[0])

    def half_rows(source, part, i):
        start = source * sqkv.shape[0] + (part * half + i) * small
        return pl.ds(pl.multiple_of(start, small), small)

    def direct(k, i, source):
        return pltpu.make_async_remote_copy(
            src_ref=sqkv.at[pl.ds(pl.multiple_of((parity * half + i) * small, small), small)],
            dst_ref=wsq.at[half_rows(source, parity, i)],
            send_sem=w_send.at[0, k, i],
            recv_sem=w_recv.at[0, k, i],
            device_id={"fsdp": (f + 2 * (k + 1)) % n_f},
            device_id_type=MESH,
        )

    def cross(k, i, source, part):
        return pltpu.make_async_remote_copy(
            src_ref=wsq.at[half_rows(source, part, i)],
            dst_ref=wsq.at[half_rows(source, part, i)],
            send_sem=w_send.at[0, k, half + i],
            recv_sem=w_recv.at[0, k, half + i],
            device_id={"tm": partner},
            device_id_type=MESH,
        )

    def half_forward(k, i, source, part, slot):
        return pltpu.make_async_remote_copy(
            src_ref=wsq.at[half_rows(source, part, i)],
            dst_ref=wsq.at[half_rows(source, part, i)],
            send_sem=m_send.at[0, k, slot],
            recv_sem=m_recv.at[0, k, slot],
            device_id={"fsdp": mate},
            device_id_type=MESH,
        )

    def source_of(who, k):
        return (who + n_f - 2 * (k + 1)) % n_f

    def relay_first():
        for i in range(half + 1):
            for k in range(peers):
                source = source_of(f, k)
                if i < half:
                    direct(k, i, source).wait_recv()
                    for cp in (
                        cross(k, i, source, parity),
                        half_forward(k, i, source, parity, i),
                    ):
                        cp.start()
                        sends.append(cp)
                if i > 0:
                    cross(k, i - 1, source, 1 - parity).wait_recv()
                    cp = half_forward(k, i - 1, source, 1 - parity, half + i - 1)
                    cp.start()
                    sends.append(cp)

    def gathered_first():
        own_weights[0].wait()
        mate_own(0, mate).wait_recv()
        for i in range(half):
            for k in range(peers):
                source = source_of(mate, k)
                half_forward(k, i, source, parity, i).wait_recv()
                half_forward(k, i, source, 1 - parity, half + i).wait_recv()

    for w, (src, dst) in enumerate(weights):
        for p in range(half if w == 0 else pieces_of(src.shape[0])):
            for k in range(peers):
                cp = direct(k, p, f) if w == 0 else peer_copy(w, k, p, f)
                cp.start()
                sends.append(cp)
        cp = mate_own(w, f)
        cp.start()
        sends.append(cp)

    def relay(w):
        for p in range(pieces_of(weights[w][0].shape[0])):
            for k in range(peers):
                source = (f + n_f - 2 * (k + 1)) % n_f
                peer_copy(w, k, p, source).wait_recv()
                cp = mate_forward(w, k, p, source)
                cp.start()
                sends.append(cp)

    def gathered(w):
        own_weights[w].wait()
        mate_own(w, mate).wait_recv()
        for p in range(pieces_of(weights[w][0].shape[0])):
            for k in range(peers):
                mate_forward(w, k, p, (mate + n_f - 2 * (k + 1)) % n_f).wait_recv()

    def norm(values, gain):
        centre = values - jnp.mean(values, axis=-1, keepdims=True)
        spread = jnp.mean(centre * centre, axis=-1, keepdims=True)
        return (centre * lax.rsqrt(spread + EPSILON) * gain).astype(BF16)

    def project(c, weight):
        tile = inner

        @pl.loop(0, weight.shape[1] // tile)
        def _(i):
            cols = pl.ds(pl.multiple_of(i * tile, LANES), tile)
            part = jnp.dot(normed[c], weight[:, cols], preferred_element_type=F32)
            proj[c, :, :, cols] = part.reshape(n_t, places, tile)

    def attend(c, lo, group, count, masked, store):
        size = n_t * group
        lane = lax.broadcasted_iota(jnp.int32, (1, LANES), 1)
        first = lane < HEAD

        if masked:
            r = lax.rem(lax.broadcasted_iota(jnp.int32, (size, 1), 0), group)
            l = lax.rem(lax.broadcasted_iota(jnp.int32, (1, size), 1), group)
            same_place = r == l

        @pl.loop(0, inner // LANES, unroll=2)
        def _(i):
            def read(offset):
                cols = pl.ds(pl.multiple_of(offset + i * LANES, LANES), LANES)
                return proj[c, :, lo : lo + group, cols].reshape(size, LANES)

            q = read(0) * HEAD ** (-0.5)
            k = read(inner)
            v = read(2 * inner).astype(BF16)
            kh = k.astype(BF16)
            kl = (k - kh.astype(F32)).astype(BF16)
            kk = jnp.concatenate([kh, kh], axis=1)
            parts = []
            for h in range(LANES // HEAD):
                qm = jnp.where(first == (h == 0), q, 0.0)
                qh = qm.astype(BF16)
                ql = (qm - qh.astype(F32)).astype(BF16)
                qq = jnp.concatenate([qh, ql], axis=1)
                dims = (((1,), (1,)), ((), ()))
                s = lax.dot_general(qq, kk, dims, preferred_element_type=F32)
                s = s + lax.dot_general(qh, kl, dims, preferred_element_type=F32)
                if masked:
                    s = jnp.where(same_place, s, -1e30)
                e = jnp.exp(s - jnp.max(s, axis=-1, keepdims=True))
                total = jnp.sum(e, axis=-1, keepdims=True)
                pv = jnp.dot(e.astype(BF16), v, preferred_element_type=F32)
                parts.append(pv / total)
            result = jnp.where(first, parts[0], parts[1])
            store(pl.ds(pl.multiple_of(i * LANES, LANES), LANES), result)

    def a2a(c, j, slot_from, send):
        to = (t + j) % n_t
        return pltpu.make_async_remote_copy(
            src_ref=mid.at[c, to],
            dst_ref=arrived.at[c, slot_from],
            send_sem=a_send.at[c, j],
            recv_sem=a_recv.at[c, j],
            device_id={"tm": to},
            device_id_type=MESH,
        )

    def back(c, j, slot_from):
        to = (t + j) % n_t
        return pltpu.make_async_remote_copy(
            src_ref=ctx_t.at[c, to],
            dst_ref=ctx_back.at[c, slot_from],
            send_sem=c_send.at[c, j],
            recv_sem=c_recv.at[c, j],
            device_id={"tm": to},
            device_id_type=MESH,
        )

    token_copy.wait()
    block = min(rows, 64)
    for c in range(clips):

        @pl.loop(0, rows // block)
        def _(i):
            where = pl.ds(pl.multiple_of(i * block, block), block)
            normed[c, where] = norm(xv[c, where].astype(F32), sg[...])

    relay_first()
    gathered_first()
    for c in range(clips):
        project(c, wsq)
    own_copies = []
    for c in range(clips):

        def store_spatial(cols, result):
            ctx[:, cols] = result.astype(BF16)

        attend(c, 0, places, 1, False, store_spatial)
        if c == 0:
            relay(1)
            gathered(1)

        @pl.loop(0, width // inner)
        def _(i):
            cols = pl.ds(pl.multiple_of(i * inner, LANES), inner)
            part = xv[c, :, cols].astype(F32) + jnp.dot(
                ctx[...], wso[:, cols], preferred_element_type=F32
            )
            mid[c, :, :, cols] = part.reshape(n_t, places, inner).astype(BF16)

        for j in range(1, n_t):
            cp = a2a(c, j, t, True)
            cp.start()
            sends.append(cp)
        cp = pltpu.make_async_copy(mid.at[c, t], arrived.at[c, t], own_sem.at[0, c])
        cp.start()
        own_copies.append(cp)

    relay(2)
    own_back = []
    group = min(places, 16)
    for c in range(clips):
        own_copies[c].wait()
        for j in range(1, n_t):
            a2a(c, j, (t + n_t - j) % n_t, False).wait_recv()
        step = max(1, block // places)

        @pl.loop(0, n_t // step)
        def _(i):
            values = arrived[c, pl.ds(i * step, step)].astype(F32).reshape(step * places, width)
            where = pl.ds(pl.multiple_of(i * step * places, step * places), step * places)
            normed[c, where] = norm(values, tg[...])

        if c == 0:
            gathered(2)
        project(c, wtq)
        for g in range(places // group):

            def store_temporal(cols, result):
                ctx_t[c, :, g * group : (g + 1) * group, cols] = result.reshape(
                    n_t, group, LANES
                ).astype(BF16)

            attend(c, g * group, group, n_t, True, store_temporal)
        for j in range(1, n_t):
            cp = back(c, j, t)
            cp.start()
            sends.append(cp)
        cp = pltpu.make_async_copy(ctx_t.at[c, t], ctx_back.at[c, t], own_sem.at[1, c])
        cp.start()
        own_back.append(cp)
        if c == 0:
            relay(3)
    gathered(3)
    finals = []
    for c in range(clips):
        own_back[c].wait()
        for j in range(1, n_t):
            back(c, j, (t + n_t - j) % n_t).wait_recv()
        ctx[...] = ctx_back[c].astype(F32).reshape(rows, inner).astype(BF16)

        @pl.loop(0, width // inner)
        def _(i):
            cols = pl.ds(pl.multiple_of(i * inner, LANES), inner)
            part = mid[c, :, :, cols].astype(F32).reshape(rows, inner) + jnp.dot(
                ctx[...], wto[:, cols], preferred_element_type=F32
            )
            outv[c, :, cols] = part.astype(BF16)

        cp = pltpu.make_async_copy(outv.at[c], out.at[c], out_sem.at[c])
        cp.start()
        finals.append(cp)
    for cp in sends:
        cp.wait_send()
    for cp in finals:
        cp.wait()


def shards(
    n_f, n_t, tokens, spatial_gain, spatial_qkv, spatial_out, temporal_gain, temporal_qkv,
    temporal_out,
):
    clip_count, frames, rows, width = tokens.shape
    assert frames == 1
    inner = spatial_out.shape[0] * n_f
    columns = spatial_qkv.shape[1]
    places = rows // n_t
    peers = max(1, n_f // 2 - 1)
    most = pieces_of(max(spatial_qkv.shape[0], spatial_out.shape[0]))
    anywhere = pl.BlockSpec(memory_space=pl.ANY)
    vmem = pl.BlockSpec(memory_space=pltpu.VMEM)
    dma = pltpu.SemaphoreType.DMA
    result = pl.pallas_call(
        functools.partial(kernel, n_f, n_t),
        out_shape=jax.ShapeDtypeStruct((clip_count, rows, width), BF16),
        in_specs=[anywhere, vmem, anywhere, anywhere, vmem, anywhere, anywhere],
        out_specs=anywhere,
        scratch_shapes=[
            pltpu.VMEM((clip_count, rows, width), BF16),
            pltpu.VMEM((clip_count, rows, width), BF16),
            pltpu.VMEM((clip_count, n_t, places, columns), F32),
            pltpu.VMEM((rows, inner), BF16),
            pltpu.VMEM((clip_count, n_t, places, width), BF16),
            pltpu.VMEM((clip_count, n_t, places, width), BF16),
            pltpu.VMEM((clip_count, n_t, places, inner), BF16),
            pltpu.VMEM((clip_count, n_t, places, inner), BF16),
            pltpu.VMEM((width, columns), BF16),
            pltpu.VMEM((inner, width), BF16),
            pltpu.VMEM((width, columns), BF16),
            pltpu.VMEM((inner, width), BF16),
            pltpu.VMEM((clip_count, rows, width), BF16),
            dma,
            dma((4,)),
            dma((4, peers, most)),
            dma((4, peers, most)),
            dma((4, peers, most)),
            dma((4, peers, most)),
            dma((4,)),
            dma((4,)),
            dma((clip_count, n_t)),
            dma((clip_count, n_t)),
            dma((clip_count, n_t)),
            dma((clip_count, n_t)),
            dma((2, clip_count)),
            dma((clip_count,)),
        ],
        compiler_params=pltpu.CompilerParams(
            collective_id=0, has_side_effects=True, vmem_limit_bytes=67000000
        ),
    )(
        tokens.reshape(clip_count, rows, width),
        spatial_gain.reshape(1, width),
        spatial_qkv,
        spatial_out,
        temporal_gain.reshape(1, width),
        temporal_qkv,
        temporal_out,
    )
    return result.reshape(clip_count, frames, rows, width)


def solution(mesh):
    placed = (
        P("fsdp", "tm", None, None),
        P(),
        P("fsdp", None),
        P("fsdp", None),
        P(),
        P("fsdp", None),
        P("fsdp", None),
    )
    body = functools.partial(shards, mesh.shape["fsdp"], mesh.shape["tm"])
    return jax.shard_map(
        body, mesh=mesh, in_specs=placed, out_specs=P("fsdp", "tm", None, None), check_vma=False
    )
```
